32 devices in a mesh: dp: 8 (over y, x, core), tp: 4 (over z).
Axes of the slice: x: 2, y: 2, z: 4, core: 2. Of those that a mesh axis runs over, the one named last changes fastest.
Arguments:
- tokens: bfloat16 [128, 8192], P('tp', 'dp'), may hold values from -6 to 6
- targets: bfloat16 [128, 8192], P('tp', 'dp'), may hold values from -6 to 6
- gate_weight: bfloat16 [8192, 16384], P('dp', 'tp'), may hold values from -0.0625 to 0.0625
- up_weight: bfloat16 [8192, 16384], P('dp', 'tp'), may hold values from -0.0625 to 0.0625
- down_weight: bfloat16 [16384, 8192], P('tp', 'dp'), may hold values from -0.046875 to 0.046875
- direction_gate: bfloat16 [8192, 16384], P('dp', 'tp'), may hold values from -36 to 36
- direction_up: bfloat16 [8192, 16384], P('dp', 'tp'), may hold values from -36 to 36
- direction_down: bfloat16 [16384, 8192], P('tp', 'dp'), may hold values from -36 to 36
- previous_gate: bfloat16 [8192, 16384], P('dp', 'tp'), may hold values from -36 to 36
- previous_up: bfloat16 [8192, 16384], P('dp', 'tp'), may hold values from -36 to 36
- previous_down: bfloat16 [16384, 8192], P('tp', 'dp'), may hold values from -36 to 36
- beta_prev: float32 [1], replicated, may hold values from 1 to 4
Outputs:
- next_gate: bfloat16 [8192, 16384], P('dp', 'tp')
- next_up: bfloat16 [8192, 16384], P('dp', 'tp')
- next_down: bfloat16 [16384, 8192], P('tp', 'dp')
- coefficients: float32 [2], replicated
The draws below stay inside these ranges and needn't reach their ends.
All inputs are finite; a program needn't handle non-finite values.
Results may differ from the reference program's by a relative error of at most 0.015.
Values may be sent and summed in bfloat16 or wider, within the bound.
A program may use at most 256 MiB of HBM per device.

```python
import math
import jax
import jax.numpy as jnp
from jax import lax

D = 8192
FF = 16384
TOKENS = 128


def rising_field(key, salt, rows, cols, width_dim):
    sub = jax.random.fold_in(key, salt)
    base = jnp.clip(jax.random.normal(sub, (rows, cols), jnp.float32), -6.0, 6.0)
    ratio = 6.0
    count = rows if width_dim == 0 else cols
    place = jnp.arange(count, dtype=jnp.float32) / max(count - 1, 1)
    factor = jnp.exp(place * math.log(ratio))
    if width_dim == 0:
        return (base * factor[:, None]).astype(jnp.bfloat16)
    return (base * factor[None, :]).astype(jnp.bfloat16)


def draw_direction_gate(key, part):
    return rising_field(key, 11, D, FF, 0)


def draw_direction_up(key, part):
    return rising_field(key, 12, D, FF, 0)


def draw_direction_down(key, part):
    return rising_field(key, 13, FF, D, 1)


def draw_previous_gate(key, part):
    return rising_field(key, 21, D, FF, 0)


def draw_previous_up(key, part):
    return rising_field(key, 22, D, FF, 0)


def draw_previous_down(key, part):
    return rising_field(key, 23, FF, D, 1)


def level_of(rng, dims, split, low, high):
    def one(position, blocks):
        steps = jax.random.uniform(jax.random.fold_in(jax.random.fold_in(rng, 6), position), (blocks,), jnp.float32, low / len(split), high / len(split))
        return jnp.repeat(jnp.exp(steps), dims[position] // blocks).reshape((-1,) + (1,) * (len(dims) - position - 1))

    loudness = one(*split[0])
    for cut in split[1:]:
        loudness = loudness * one(*cut)
    return loudness


def gaussian(own_key, dims, spread, most, split=(), kind=jnp.bfloat16):
    gain = level_of(own_key, dims, split, -0.22, 0.18) if split else 1.0
    values = jax.random.normal(own_key, dims, jnp.float32) * spread * gain
    return jnp.minimum(jnp.maximum(values, -most), most).astype(kind)


def setup_inputs(seed: int = 0) -> dict:
    arg_keys = jax.random.split(jax.random.key(seed), 13)
    return {
        "tokens": gaussian(arg_keys[0], (TOKENS, D), 1.0, 6.0, ((0, 4), (1, 8))),
        "targets": gaussian(arg_keys[1], (TOKENS, D), 1.0, 6.0, ((0, 4), (1, 8))),
        "gate_weight": gaussian(arg_keys[2], (D, FF), D ** -0.5, 0.0625, ((0, 8), (1, 4))),
        "up_weight": gaussian(arg_keys[3], (D, FF), D ** -0.5, 0.0625, ((0, 8), (1, 4))),
        "down_weight": gaussian(arg_keys[4], (FF, D), FF ** -0.5, 0.046875, ((0, 4), (1, 8))),
        "direction_gate": draw_direction_gate(jax.random.fold_in(arg_keys[12], 71), 0),
        "direction_up": draw_direction_up(jax.random.fold_in(arg_keys[12], 71), 0),
        "direction_down": draw_direction_down(jax.random.fold_in(arg_keys[12], 71), 0),
        "previous_gate": draw_previous_gate(jax.random.fold_in(arg_keys[12], 71), 0),
        "previous_up": draw_previous_up(jax.random.fold_in(arg_keys[12], 71), 0),
        "previous_down": draw_previous_down(jax.random.fold_in(arg_keys[12], 71), 0),
        "beta_prev": jnp.clip(jax.random.uniform(arg_keys[11], (1,), jnp.float32, 1.0, 4.0), 1.0, 4.0),
    }


def product(first_op, second_op):
    return jnp.dot(first_op, second_op, preferred_element_type=jnp.float32)

def against(first_op, second_op):
    return lax.dot_general(first_op, second_op, (((1,), (1,)), ((), ())), preferred_element_type=jnp.float32)

def transposed(first_op, second_op):
    return lax.dot_general(first_op, second_op, (((0,), (0,)), ((), ())), preferred_element_type=jnp.float32)

def pointwise(gate_sum):
    logistic = jax.nn.sigmoid(gate_sum)
    activation = gate_sum * logistic
    gate_slope = logistic * (1.0 + gate_sum * (1.0 - logistic))
    gate_curve = logistic * (1.0 - logistic) * (2.0 + gate_sum * (1.0 - 2.0 * logistic))
    return (activation, gate_slope, gate_curve)

def reference(tokens, targets, gate_weight, up_weight, down_weight, direction_gate, direction_up, direction_down, previous_gate, previous_up, previous_down, beta_prev):
    gate_sum = product(tokens, gate_weight)
    up_sum = product(tokens, up_weight)
    gate_dir = product(tokens, direction_gate)
    up_dir = product(tokens, direction_up)
    activation, gate_slope, gate_curve = pointwise(gate_sum)
    hidden = (activation * up_sum).astype(jnp.bfloat16)
    hidden_dir = (gate_slope * up_sum * gate_dir + activation * up_dir).astype(jnp.bfloat16)
    output = product(hidden, down_weight)
    output_dir = product(hidden_dir, down_weight) + product(hidden, direction_down)
    total_rows = tokens.shape[0]
    grad_out = ((output - targets.astype(jnp.float32)) / total_rows).astype(jnp.bfloat16)
    grad_out_dir = (output_dir / total_rows).astype(jnp.bfloat16)
    grad_hidden = against(grad_out, down_weight)
    grad_hidden_dir = against(grad_out_dir, down_weight) + against(grad_out, direction_down)
    grad_gate_dir = (grad_hidden_dir * up_sum * gate_slope + grad_hidden * up_dir * gate_slope + grad_hidden * up_sum * gate_curve * gate_dir).astype(jnp.bfloat16)
    grad_up_dir = (grad_hidden_dir * activation + grad_hidden * gate_slope * gate_dir).astype(jnp.bfloat16)
    image_gate = transposed(tokens, grad_gate_dir)
    image_up = transposed(tokens, grad_up_dir)
    image_down = transposed(hidden_dir, grad_out) + transposed(hidden, grad_out_dir)
    images = [image_gate, image_up, image_down]
    alongs = [matrix.astype(jnp.float32) for matrix in (direction_gate, direction_up, direction_down)]
    befores = [matrix.astype(jnp.float32) for matrix in (previous_gate, previous_up, previous_down)]
    entries = 3 * D * FF
    alpha_coef = sum((jnp.sum(image_part * along_part) for image_part, along_part in zip(images, alongs))) / entries
    beta_old = beta_prev[0]
    residuals = [image_part - alpha_coef * along_part - beta_old * before_part for image_part, along_part, before_part in zip(images, alongs, befores)]
    beta_coef = jnp.sqrt(sum((jnp.sum(matrix * matrix) for matrix in residuals)) / entries + 1e-06)
    next_parts = [(matrix / beta_coef).astype(jnp.bfloat16) for matrix in residuals]
    return (next_parts[0], next_parts[1], next_parts[2], jnp.stack([alpha_coef, beta_coef]).astype(jnp.float32))
```

```python
import functools

import jax
import jax.numpy as jnp
from jax import lax
from jax.experimental import pallas as pl
from jax.experimental.pallas import tpu as pltpu
from jax.sharding import PartitionSpec as P

MESH = pl.DeviceIdType.MESH
VMEM = pltpu.VMEM
DMA = pltpu.SemaphoreType.DMA
F32 = jnp.float32
BF16 = jnp.bfloat16
LIMIT = 56 * 1024 * 1024


def tile_of(size, most):
    tile = min(size, most)
    while size % tile:
        tile //= 2
    return tile


def greet(targets):
    barrier = pltpu.get_barrier_semaphore()
    for target in targets:
        pl.semaphore_signal(barrier, inc=1, device_id=target, device_id_type=MESH)
    pl.semaphore_wait(barrier, len(targets))


def send(src, dst, send_sem, recv_sem, target):
    copy = pltpu.make_async_remote_copy(
        src_ref=src, dst_ref=dst, send_sem=send_sem, recv_sem=recv_sem, device_id=target, device_id_type=MESH
    )
    copy.start()
    return copy


def by_columns(width, body):
    step = tile_of(width, 512)

    @pl.loop(0, width // step)
    def _(i):
        body(pl.ds(pl.multiple_of(i * step, step), step))


def forward_rows(parts, keeps, cols):
    gate_sum, up_sum, gate_dir, up_dir = parts
    for keep, part in zip(keeps, parts):
        keep[:, cols] = part
    logistic = jax.nn.sigmoid(gate_sum)
    activation = gate_sum * logistic
    gate_slope = logistic * (1.0 + gate_sum * (1.0 - logistic))
    hidden = activation * up_sum
    hidden_dir = gate_slope * up_sum * gate_dir + activation * up_dir
    return hidden, hidden_dir


def backward_rows(parts, keeps, cols):
    grad_hidden, grad_hidden_dir = parts
    gate_sum, up_sum, gate_dir, up_dir = (keep[:, cols] for keep in keeps)
    logistic = jax.nn.sigmoid(gate_sum)
    activation = gate_sum * logistic
    gate_slope = logistic * (1.0 + gate_sum * (1.0 - logistic))
    gate_curve = logistic * (1.0 - logistic) * (2.0 + gate_sum * (1.0 - 2.0 * logistic))
    grad_gate = (
        grad_hidden_dir * up_sum * gate_slope
        + grad_hidden * up_dir * gate_slope
        + grad_hidden * up_sum * gate_curve * gate_dir
    )
    grad_up = grad_hidden_dir * activation + grad_hidden * gate_slope * gate_dir
    return grad_gate, grad_up


def width_kernel(n, kinds, rows_of, keeps_in, *refs):
    x = refs[0]
    if keeps_in:
        keeps, out = refs[1:5], refs[5]
    else:
        out, keeps = refs[1], refs[2:6]
    mate_in, paired, far_in, full, s1, r1, s2, r2, s3, r3, s4, r4, local = refs[6:]
    chips = n // 2
    width = x.shape[-1]
    me = lax.axis_index("dp")
    chip, core = lax.div(me, 2), lax.rem(me, 2)
    mate = {"dp": me + 1 - 2 * core}
    afar = [{"dp": lax.rem(chip + s, chips) * 2 + core} for s in range(1, chips)]
    greet([mate] + afar)

    order = list(range(1, chips)) + [0]
    spot = [lax.rem(chip + s, chips) for s in range(chips)]
    source = [lax.rem(chip + chips - s, chips) for s in range(chips)]
    first = {
        s: send(x.at[:, spot[s], 1 - core], mate_in.at[:, spot[s]], s1.at[s], r1.at[s], mate)
        for s in order
    }
    second = {}
    for s in order:
        first[s].wait_recv()

        def pair(cols, s=s):
            for kind in range(kinds):
                paired[kind, spot[s], :, cols] = (
                    x[kind, spot[s], core, :, cols].astype(F32)
                    + mate_in[kind, spot[s], :, cols].astype(F32)
                ).astype(BF16)

        by_columns(width, pair)
        if s:
            second[s] = send(
                paired.at[:, spot[s]], far_in.at[:, chip], s2.at[s], r2.at[s], afar[s - 1]
            )
    for s in range(1, chips):
        second[s].wait_recv()

    def finish(cols):
        parts = []
        for kind in range(kinds):
            total = paired[kind, chip, :, cols].astype(F32)
            for s in range(1, chips):
                total = total + far_in[kind, source[s], :, cols].astype(F32)
            parts.append(total)
        one, two = rows_of(parts, keeps, cols)
        full[0, me, :, cols] = one.astype(BF16)
        full[1, me, :, cols] = two.astype(BF16)

    by_columns(width, finish)

    mine = full.at[:, me]
    third = [send(mine, mine, s3.at[s], r3.at[s], afar[s - 1]) for s in range(1, chips)]
    fourth = [send(mine, mine, s4.at[0], r4.at[0], mate)]
    stores = [pltpu.make_async_copy(mine, out.at[:, me], local.at[0])]
    stores[0].start()
    for s in range(1, chips):
        third[s - 1].wait_recv()
        at = source[s] * 2 + core
        fourth.append(send(full.at[:, at], full.at[:, at], s4.at[s], r4.at[s], mate))
        store = pltpu.make_async_copy(full.at[:, at], out.at[:, at], local.at[s])
        store.start()
        stores.append(store)
    for s in range(chips):
        fourth[s].wait_recv()
        at = source[s] * 2 + 1 - core
        store = pltpu.make_async_copy(full.at[:, at], out.at[:, at], local.at[chips + s])
        store.start()
        stores.append(store)
    for copy in list(first.values()) + list(second.values()) + third + fourth:
        copy.wait_send()
    for store in stores:
        store.wait()


def width_exchange(n, x, keeps, rows_of, collective_id):
    kinds, rows, width = x.shape
    share, chips = rows // n, n // 2
    keeps_in = keeps is not None
    x = x.reshape(kinds, chips, 2, share, width)
    vmem, anywhere = pl.BlockSpec(memory_space=VMEM), pl.BlockSpec(memory_space=pl.ANY)
    out_shape = [jax.ShapeDtypeStruct((2, n, share, width), BF16)]
    out_specs = [anywhere]
    if not keeps_in:
        out_shape += [jax.ShapeDtypeStruct((share, width), F32)] * 4
        out_specs += [vmem] * 4
    slots = VMEM((kinds, chips, share, width), BF16)
    sems = DMA((chips,))
    result = pl.pallas_call(
        functools.partial(width_kernel, n, kinds, rows_of, keeps_in),
        out_shape=out_shape,
        in_specs=[vmem] * (5 if keeps_in else 1),
        out_specs=out_specs,
        scratch_shapes=[slots, slots, slots, VMEM((2, n, share, width), BF16)]
        + [sems] * 8
        + [DMA((n,))],
        compiler_params=pltpu.CompilerParams(
            collective_id=collective_id, has_side_effects=True, vmem_limit_bytes=LIMIT
        ),
    )(x, *(keeps or ()))
    return result[0].reshape(2, rows, width), tuple(result[1:])


def ring_of(t):
    me = lax.axis_index("tp")
    return me, [lax.rem(me + s, t) for s in range(1, t)], [lax.rem(me + t - s, t) for s in range(1, t)]


def tokens_kernel(t, x, out, full, ssem, rsem, local):
    me, spots, sources = ring_of(t)
    greet([{"tp": spot} for spot in spots])
    copies = [
        send(x, full.at[me], ssem.at[i], rsem.at[i], {"tp": spot}) for i, spot in enumerate(spots)
    ]
    stores = [pltpu.make_async_copy(x, out.at[me], local.at[t - 1])]
    stores[0].start()
    for i, copy in enumerate(copies):
        copy.wait_recv()
        store = pltpu.make_async_copy(full.at[sources[i]], out.at[sources[i]], local.at[i])
        store.start()
        stores.append(store)
    for copy in copies:
        copy.wait_send()
    for store in stores:
        store.wait()


def tokens_exchange(t, x):
    share, width = x.shape
    out = pl.pallas_call(
        functools.partial(tokens_kernel, t),
        out_shape=jax.ShapeDtypeStruct((t, share, width), BF16),
        in_specs=[pl.BlockSpec(memory_space=VMEM)],
        out_specs=pl.BlockSpec(memory_space=pl.ANY),
        scratch_shapes=[VMEM((t, share, width), BF16), DMA((t - 1,)), DMA((t - 1,)), DMA((t,))],
        compiler_params=pltpu.CompilerParams(
            collective_id=1, has_side_effects=True, vmem_limit_bytes=LIMIT
        ),
    )(x)
    return out.reshape(t * share, width)


def output_kernel(t, x, targets, out, far_in, full, s1, r1, s2, r2, local):
    me, spots, sources = ring_of(t)
    share, width = targets.shape
    rows = t * share
    greet([{"tp": spot} for spot in spots])
    first = [
        send(x.at[:, spot], far_in.at[:, me], s1.at[i], r1.at[i], {"tp": spot})
        for i, spot in enumerate(spots)
    ]
    for copy in first:
        copy.wait_recv()

    def finish(cols):
        parts = []
        for kind in range(2):
            total = x[kind, me, :, cols].astype(F32)
            for at in sources:
                total = total + far_in[kind, at, :, cols].astype(F32)
            parts.append(total)
        full[0, me, :, cols] = ((parts[0] - targets[:, cols].astype(F32)) / rows).astype(BF16)
        full[1, me, :, cols] = (parts[1] / rows).astype(BF16)

    by_columns(width, finish)
    mine = full.at[:, me]
    second = [
        send(mine, mine, s2.at[i], r2.at[i], {"tp": spot}) for i, spot in enumerate(spots)
    ]
    stores = [pltpu.make_async_copy(mine, out.at[:, me], local.at[t - 1])]
    stores[0].start()
    for i, copy in enumerate(second):
        copy.wait_recv()
        at = sources[i]
        store = pltpu.make_async_copy(full.at[:, at], out.at[:, at], local.at[i])
        store.start()
        stores.append(store)
    for copy in first + second:
        copy.wait_send()
    for store in stores:
        store.wait()


def output_exchange(t, x, targets):
    _, rows, width = x.shape
    share = rows // t
    vmem = pl.BlockSpec(memory_space=VMEM)
    slots = VMEM((2, t, share, width), BF16)
    out = pl.pallas_call(
        functools.partial(output_kernel, t),
        out_shape=jax.ShapeDtypeStruct((2, t, share, width), BF16),
        in_specs=[vmem, vmem],
        out_specs=pl.BlockSpec(memory_space=pl.ANY),
        scratch_shapes=[slots, slots] + [DMA((t - 1,))] * 4 + [DMA((t,))],
        compiler_params=pltpu.CompilerParams(
            collective_id=2, has_side_effects=True, vmem_limit_bytes=LIMIT
        ),
    )(x.reshape(2, t, share, width), targets)
    return out.reshape(2, rows, width)


def totals_kernel(n, t, x, out, dp_in, sums, tp_in, s1, r1, s2, r2, local):
    dp, tp = lax.axis_index("dp"), lax.axis_index("tp")
    dp_spots = [lax.rem(dp + s, n) for s in range(1, n)]
    tp_spots = [lax.rem(tp + s, t) for s in range(1, t)]
    greet([{"dp": spot} for spot in dp_spots] + [{"tp": spot} for spot in tp_spots])
    first = [
        send(x, dp_in.at[dp], s1.at[i], r1.at[i], {"dp": spot}) for i, spot in enumerate(dp_spots)
    ]
    dp_in[dp] = x[...]
    for copy in first:
        copy.wait_recv()
    total = dp_in[0]
    for at in range(1, n):
        total = total + dp_in[at]
    sums[...] = total
    tp_in[tp] = total
    second = [
        send(sums, tp_in.at[tp], s2.at[i], r2.at[i], {"tp": spot})
        for i, spot in enumerate(tp_spots)
    ]
    for copy in second:
        copy.wait_recv()
    total = tp_in[0]
    for at in range(1, t):
        total = total + tp_in[at]
    out[...] = total
    for copy in first + second:
        copy.wait_send()


def totals_exchange(n, t, x):
    vmem = pl.BlockSpec(memory_space=VMEM)
    rows, lanes = x.shape
    return pl.pallas_call(
        functools.partial(totals_kernel, n, t),
        out_shape=jax.ShapeDtypeStruct((rows, lanes), F32),
        in_specs=[vmem],
        out_specs=vmem,
        scratch_shapes=[
            VMEM((n, rows, lanes), F32),
            VMEM((rows, lanes), F32),
            VMEM((t, rows, lanes), F32),
            DMA((n - 1,)),
            DMA((n - 1,)),
            DMA((t - 1,)),
            DMA((t - 1,)),
            DMA((1,)),
        ],
        compiler_params=pltpu.CompilerParams(collective_id=3, has_side_effects=True),
    )(x)


def squares(along_ref, before_ref, norms):
    rows, width = along_ref.shape
    step = tile_of(rows, 32)

    def body(i, sums):
        at = pl.ds(pl.multiple_of(i * step, step), step)
        along = along_ref[at, :].astype(F32)
        before = before_ref[at, :].astype(F32)
        products = (along * along, along * before, before * before)
        return tuple(
            have + product.reshape(step // 8, 8, width).sum(axis=0)
            for have, product in zip(sums, products)
        )

    zero = jnp.zeros((8, width), F32)
    sums = lax.fori_loop(0, rows // step, body, (zero, zero, zero))
    for kind in range(3):
        norms[kind] += sums[kind]


def dot(one, two):
    return jnp.dot(one, two, preferred_element_type=F32)


def front_kernel(tokens, gate, up, along_gate, along_up, before_gate, before_up, x, before, norms):
    @pl.when(pl.program_id(0) == 0)
    def _():
        norms[...] = jnp.zeros_like(norms)

    rows = tokens[...]
    for kind, ref in enumerate((gate, up, along_gate, along_up)):
        x[kind] = dot(rows, ref[...]).astype(BF16)
    for kind, ref in enumerate((before_gate, before_up)):
        before[kind] = dot(rows, ref[...]).astype(BF16)
    squares(along_gate, before_gate, norms)
    squares(along_up, before_up, norms)


def front_products(tokens, *matrices):
    rows, depth = tokens.shape
    width = matrices[0].shape[1]
    tile = tile_of(width, 512)
    return pl.pallas_call(
        front_kernel,
        grid=(width // tile,),
        out_shape=(
            jax.ShapeDtypeStruct((4, rows, width), BF16),
            jax.ShapeDtypeStruct((2, rows, width), BF16),
            jax.ShapeDtypeStruct((3, 8, tile), F32),
        ),
        in_specs=[pl.BlockSpec((rows, depth), lambda i: (0, 0))]
        + [pl.BlockSpec((depth, tile), lambda i: (0, i))] * 6,
        out_specs=(
            pl.BlockSpec((4, rows, tile), lambda i: (0, 0, i)),
            pl.BlockSpec((2, rows, tile), lambda i: (0, 0, i)),
            pl.BlockSpec((3, 8, tile), lambda i: (0, 0, 0)),
        ),
        compiler_params=pltpu.CompilerParams(vmem_limit_bytes=LIMIT),
    )(tokens, *matrices)


def middle_kernel(units, down, along, before, weighted, moved, was, norms):
    @pl.when(pl.program_id(0) == 0)
    def _():
        for ref in (weighted, moved, was, norms):
            ref[...] = jnp.zeros_like(ref)

    rows = units[...]
    weighted[...] += dot(rows, down[...])
    moved[...] += dot(rows, along[...])
    was[...] += dot(rows, before[...])
    squares(along, before, norms)


def middle_products(units, down, along, before):
    rows, depth = units.shape
    width = down.shape[1]
    tile = tile_of(depth, 512)
    whole = pl.BlockSpec((rows, width), lambda i: (0, 0))
    return pl.pallas_call(
        middle_kernel,
        grid=(depth // tile,),
        out_shape=[jax.ShapeDtypeStruct((rows, width), F32)] * 3
        + [jax.ShapeDtypeStruct((3, 8, width), F32)],
        in_specs=[pl.BlockSpec((rows, tile), lambda i: (0, i))]
        + [pl.BlockSpec((tile, width), lambda i: (i, 0))] * 3,
        out_specs=[whole] * 3 + [pl.BlockSpec((3, 8, width), lambda i: (0, 0, 0))],
        compiler_params=pltpu.CompilerParams(vmem_limit_bytes=LIMIT),
    )(units, down, along, before)


def against(one, two):
    return lax.dot_general(one, two, (((1,), (1,)), ((), ())), preferred_element_type=F32)


def transposed(one, two):
    return lax.dot_general(one, two, (((0,), (0,)), ((), ())), preferred_element_type=F32)


def back_kernel(grads, down, along, x):
    rows = grads.shape[0] // 2
    weighted = against(grads[...], down[...])
    moved = against(grads[:rows, :], along[...])
    x[0] = weighted[:rows].astype(BF16)
    x[1] = (weighted[rows:] + moved).astype(BF16)


def back_products(grads, down, along):
    rows, depth = grads.shape
    width = down.shape[0]
    tile = tile_of(width, 512)
    return pl.pallas_call(
        back_kernel,
        grid=(width // tile,),
        out_shape=jax.ShapeDtypeStruct((2, rows // 2, width), BF16),
        in_specs=[pl.BlockSpec((rows, depth), lambda i: (0, 0))]
        + [pl.BlockSpec((tile, depth), lambda i: (i, 0))] * 2,
        out_specs=pl.BlockSpec((2, rows // 2, tile), lambda i: (0, 0, i)),
        compiler_params=pltpu.CompilerParams(vmem_limit_bytes=LIMIT),
    )(grads, down, along)


def next_kernel(count, scales, *refs):
    one, rest = refs[0], refs[1:]
    twos, alongs, befores, outs = (rest[i * count : (i + 1) * count] for i in range(4))
    inverse, alpha, beta = scales[0], scales[1], scales[2]
    for two, along, before, out in zip(twos, alongs, befores, outs):
        image = transposed(one[...], two[...])
        out[...] = (
            image * inverse - along[...].astype(F32) * alpha - before[...].astype(F32) * beta
        ).astype(BF16)


def next_parts(scales, one, twos, alongs, befores):
    count = len(twos)
    rows, height = one.shape
    width = twos[0].shape[1]
    tile = tile_of(height, max(128, (1 << 20) // (width * count)))
    block = pl.BlockSpec((tile, width), lambda i: (i, 0))
    return pl.pallas_call(
        functools.partial(next_kernel, count),
        grid=(height // tile,),
        out_shape=[jax.ShapeDtypeStruct((height, width), BF16)] * count,
        in_specs=[pl.BlockSpec(memory_space=pltpu.SMEM), pl.BlockSpec((rows, tile), lambda i: (0, i))]
        + [pl.BlockSpec((rows, width), lambda i: (0, 0))] * count
        + [block] * (2 * count),
        out_specs=[block] * count,
        compiler_params=pltpu.CompilerParams(vmem_limit_bytes=LIMIT),
    )(scales, one, *twos, *alongs, *befores)


def on_device(
    n,
    t,
    tokens,
    targets,
    gate_weight,
    up_weight,
    down_weight,
    direction_gate,
    direction_up,
    direction_down,
    previous_gate,
    previous_up,
    previous_down,
    beta_prev,
):
    everyone = tokens_exchange(t, tokens)
    rows = everyone.shape[0]
    x, before, norms = front_products(
        everyone, gate_weight, up_weight, direction_gate, direction_up, previous_gate, previous_up
    )
    units, keeps = width_exchange(n, x, None, forward_rows, 4)
    units = units.reshape(2 * rows, -1)
    weighted, moved, was, down_norms = middle_products(
        units, down_weight, direction_down, previous_down
    )
    outputs = jnp.stack([weighted[:rows], weighted[rows:] + moved[:rows]]).astype(BF16)
    grads = output_exchange(t, outputs, targets)
    grads = grads.reshape(2 * rows, -1)
    y = back_products(grads, down_weight, direction_down)
    dirs, _ = width_exchange(n, y, keeps, backward_rows, 5)

    swapped = jnp.concatenate([units[rows:], units[:rows]])
    gram = against(dirs[0], dirs[0]) + against(dirs[1], dirs[1])
    image_image = jnp.sum(against(everyone, everyone) * gram) + jnp.sum(
        against(swapped, swapped) * against(grads, grads)
    )
    swapped_moved = jnp.concatenate([moved[rows:], moved[:rows]])
    swapped_was = jnp.concatenate([was[rows:], was[:rows]])
    wide = dirs.astype(F32)
    tall = grads.astype(F32)
    image_along = jnp.sum(wide * x[2:].astype(F32)) + jnp.sum(tall * swapped_moved)
    image_before = jnp.sum(wide * before.astype(F32)) + jnp.sum(tall * swapped_was)
    own = jnp.sum(norms, axis=(1, 2)) + jnp.sum(down_norms, axis=(1, 2))
    sums = jnp.concatenate([jnp.stack([image_image, image_along, image_before]), own])
    sums = jnp.broadcast_to(jnp.pad(sums, (0, 2))[:, None], (8, 128))
    totals = totals_exchange(n, t, sums)[:, 0]
    image_image, image_along, image_before = totals[0], totals[1], totals[2]
    along_along, along_before, before_before = totals[3], totals[4], totals[5]
    entries = float(
        n * t * (gate_weight.size + up_weight.size + down_weight.size)
    )
    beta_old = beta_prev[0]
    alpha_coef = image_along / entries
    square = (
        image_image
        - 2.0 * alpha_coef * image_along
        - 2.0 * beta_old * image_before
        + alpha_coef * alpha_coef * along_along
        + 2.0 * alpha_coef * beta_old * along_before
        + beta_old * beta_old * before_before
    )
    beta_coef = jnp.sqrt(square / entries + 1e-06)
    inverse = 1.0 / beta_coef
    scales = jnp.stack([inverse, alpha_coef * inverse, beta_old * inverse])
    next_gate, next_up = next_parts(
        scales,
        everyone,
        (dirs[0], dirs[1]),
        (direction_gate, direction_up),
        (previous_gate, previous_up),
    )
    (next_down,) = next_parts(scales, swapped, (grads,), (direction_down,), (previous_down,))
    return (next_gate, next_up, next_down, jnp.stack([alpha_coef, beta_coef]))


def solution(mesh):
    wide, tall = P("dp", "tp"), P("tp", "dp")
    in_specs = (tall, tall, wide, wide, tall, wide, wide, tall, wide, wide, tall, P())
    return jax.shard_map(
        functools.partial(on_device, mesh.shape["dp"], mesh.shape["tp"]),
        mesh=mesh,
        in_specs=in_specs,
        out_specs=(wide, wide, tall, P()),
        check_vma=False,
    )
```
